32 devices in a mesh: rel: 4 (over z), node: 2 (over x), head: 4 (over y, core).
Axes of the slice: x: 2, y: 2, z: 4, core: 2. Of those that a mesh axis runs over, the one named last changes fastest.
Arguments:
- features: bfloat16 [4096, 512], P('node'), may hold values from -26 to 26
- node_type: int32 [4096], P('node'), may hold values from 0 to 3
- w_query: bfloat16 [4, 512, 512], P(None, None, 'head'), may hold values from -0.25 to 0.25
- w_key: bfloat16 [4, 512, 512], P(None, None, 'head'), may hold values from -0.25 to 0.25
- w_value: bfloat16 [4, 512, 512], P(None, None, 'head'), may hold values from -0.25 to 0.25
- rel_att: bfloat16 [64, 8, 64, 64], P(None, 'head'), may hold values from -0.75 to 0.75
- rel_msg: bfloat16 [64, 8, 64, 64], P(None, 'head'), may hold values from -0.75 to 0.75
- rel_prior: float32 [64, 8], P(None, 'head'), may hold values from 0.5 to 3
- w_out: bfloat16 [4, 512, 512], P(None, 'head'), may hold values from -0.25 to 0.25
- skip: float32 [4], replicated, may hold values from -1.5 to 1.5
- rel_perm: int32 [64], P('rel'), may hold values from 0 to 63, each once
- tile_src: int32 [64, 32], P('rel', 'node'), may hold values from 0 to 31
- tile_dst: int32 [64, 32], P('rel', 'node'), may hold values from 0 to 15
- tile_bits: int32 [64, 32, 128, 4], P('rel', 'node'), may hold values from -2147483648 to 2147483646
- tile_count: int32 [64, 2], P('rel', 'node'), may hold values from 1 to 16, as said below
Outputs:
- updated: bfloat16 [4096, 512], P(('node', 'head'))
The draws below stay inside these ranges and needn't reach their ends.
Inputs may be any that keep to these rules, and one draw needn't show every extreme that they name: The first tile_count[p, g] slots of group g of position p are live; the words of the other slots may have bits set, but those bits give no edges and must be ignored. Some position has all 16 slots live in every group.
All inputs are finite; a program needn't handle non-finite values.
Results may differ from the reference program's by a relative error of at most 0.008.
The reference program's roundings to bfloat16 on the way (of `qrel` and `hidden`) count: a program that leaves them out, or rounds other values in their place, can miss the bound.
Values may be sent and summed in bfloat16 or wider, within the bound.
No kernel may reach another device: no remote copies, remote signals or barrier semaphores. Data moves between devices by JAX's collectives and lax.ppermute only.
A program may use at most 128 MiB of HBM per device.

```python
import math
import jax
import jax.numpy as jnp
from jax import lax

D = 512
HEADS = 8
TYPES = 4
RELS = 64
BLOCK = 128
NB_DEV = 16
TCAP = 16
HD = 64
WORDS = 4
NSHARD = 2
NBLOCKS = 32
NODES = 4096
TILE_SLOTS = 32


def draw_features(key, part):
    first = jax.random.fold_in(key, 0)
    base = jnp.clip(jax.random.normal(first, (NODES, D), jnp.float32), -6.0, 6.0)
    return base.astype(jnp.bfloat16)


def draw_tile_count(key, part):
    first, second, third = jax.random.split(key, 3)
    lowest = max(TCAP // 10, 1)
    sizes = jax.random.randint(first, (RELS, 1), lowest, TCAP + 1)
    drops = jax.random.randint(second, (RELS, NSHARD), 0, 4)
    counts = sizes - drops * sizes // 8
    chosen = jax.random.randint(third, (), 0, RELS)
    rows = jnp.arange(RELS, dtype=jnp.int32)[:, None]
    counts = jnp.where(rows == chosen, TCAP, counts)
    return jnp.maximum(counts, 1).astype(jnp.int32)


def slot_targets(key):
    return jax.random.randint(jax.random.fold_in(key, 11), (RELS, TILE_SLOTS), 0, NB_DEV).astype(jnp.int32)


def draw_tile_dst(key, part):
    return slot_targets(key)


def draw_tile_bits(key, part):
    targets = slot_targets(key)
    packed = jax.random.randint(jax.random.fold_in(key, 13), (RELS, TILE_SLOTS, BLOCK, WORDS), -2147483648, 2147483647, dtype=jnp.int32)
    marked = jax.random.randint(jax.random.fold_in(key, 17), (NBLOCKS, BLOCK), 0, 16)
    chosen = jax.random.randint(jax.random.fold_in(key, 19), (), 0, NBLOCKS * BLOCK)
    node_ids = jnp.arange(NBLOCKS * BLOCK, dtype=jnp.int32).reshape(NBLOCKS, BLOCK)
    lonely = (marked == 0) | (node_ids == chosen)
    groups = jnp.arange(TILE_SLOTS, dtype=jnp.int32) // TCAP
    blocks = (groups[None, :] * NB_DEV + targets).astype(jnp.int32)
    silenced = lonely[blocks]
    return jnp.where(silenced[..., None], 0, packed).astype(jnp.int32)


def with_ends(result, own_key, smallest, top_value):
    longest = result.shape.index(max(result.shape))
    spots = []
    for shift in (0, 1):
        where = [jax.random.randint(jax.random.fold_in(own_key, axis), (), 0, length) for axis, length in enumerate(result.shape)]
        where[longest] = (where[longest] + shift) % result.shape[longest]
        spots.append(tuple(where))
    return result.at[spots[0]].set(smallest).at[spots[1]].set(top_value)


def steps_of(rng, shape, pieces, low, largest):
    level, own = 1.0, jax.random.fold_in(rng, 6)
    for position, shards_of in pieces:
        draws = jnp.exp(jax.random.uniform(jax.random.fold_in(own, position), (shards_of,), jnp.float32, low / len(pieces), largest / len(pieces)))
        level = level * jnp.repeat(draws, shape[position] // shards_of).reshape([-1 if axis == position else 1 for axis in range(len(shape))])
    return level


def normal_values(stream_key, shape, spread, bound, cuts=(), held_as=jnp.bfloat16):
    factor_of = steps_of(stream_key, shape, cuts, -0.22, 0.18) if cuts else 1.0
    array = jax.random.normal(stream_key, shape, jnp.float32) * spread * factor_of
    return jnp.minimum(jnp.maximum(array, -bound), bound).astype(held_as)


def setup_inputs(seed: int = 0) -> dict:
    seeds = jax.random.split(jax.random.key(seed), 16)
    return {
        "features": draw_features(jax.random.fold_in(seeds[15], 71), 0),
        "node_type": with_ends(jax.random.randint(seeds[1], (NODES,), 0, TYPES), jax.random.fold_in(seeds[1], 1), 0, TYPES - 1).astype(jnp.int32),
        "w_query": normal_values(seeds[2], (TYPES, D, D), D ** -0.5, 0.25, ((2, 4),)),
        "w_key": normal_values(seeds[3], (TYPES, D, D), D ** -0.5, 0.25, ((2, 4),)),
        "w_value": normal_values(seeds[4], (TYPES, D, D), D ** -0.5, 0.25, ((2, 4),)),
        "rel_att": normal_values(seeds[5], (RELS, HEADS, HD, HD), HD ** -0.5, 0.75, ((1, 4),)),
        "rel_msg": normal_values(seeds[6], (RELS, HEADS, HD, HD), HD ** -0.5, 0.75, ((1, 4),)),
        "rel_prior": jnp.clip(jnp.exp(math.log(3.0) - 1.7917595 * jax.random.uniform(seeds[7], (RELS, HEADS), jnp.float32) ** steps_of(seeds[7], (RELS, HEADS), ((1, 4),), -0.2, 0.2)), 0.5, 3.0),
        "w_out": normal_values(seeds[8], (TYPES, D, D), D ** -0.5, 0.25, ((1, 4),)),
        "skip": jnp.clip(jax.random.uniform(seeds[9], (TYPES,), jnp.float32, -1.5, 1.5), -1.5, 1.5),
        "rel_perm": jax.random.permutation(seeds[10], RELS).astype(jnp.int32),
        "tile_src": with_ends(jax.random.randint(seeds[11], (RELS, TILE_SLOTS), 0, NBLOCKS), jax.random.fold_in(seeds[11], 1), 0, NBLOCKS - 1).astype(jnp.int32),
        "tile_dst": draw_tile_dst(jax.random.fold_in(seeds[15], 71), 0),
        "tile_bits": draw_tile_bits(jax.random.fold_in(seeds[15], 71), 0),
        "tile_count": draw_tile_count(jax.random.fold_in(seeds[15], 71), 0),
    }


NEG = -1e+30

def project(rows, types, weights):
    total = jnp.zeros((rows.shape[0], weights.shape[2]), jnp.float32)
    for kind in range(weights.shape[0]):
        partial_out = jnp.dot(rows, weights[kind], preferred_element_type=jnp.float32)
        total = jnp.where((types == kind)[:, None], partial_out, total)
    return total

def unpack(words):
    shifts = jnp.arange(32, dtype=jnp.int32)
    bits = words[..., None] >> shifts & 1
    return bits.reshape(words.shape[:-1] + (words.shape[-1] * 32,)) > 0

def reference(features, node_type, w_query, w_key, w_value, rel_att, rel_msg, rel_prior, w_out, skip, rel_perm, tile_src, tile_dst, tile_bits, tile_count):
    query = project(features, node_type, w_query).astype(jnp.bfloat16)
    key = project(features, node_type, w_key).astype(jnp.bfloat16)
    value = project(features, node_type, w_value).astype(jnp.bfloat16)
    query_f = query.reshape(NODES, HEADS, HD).astype(jnp.float32)
    key_blocks = key.reshape(NBLOCKS, BLOCK, HEADS, HD)
    value_blocks = value.reshape(NBLOCKS, BLOCK, HEADS, HD)
    factor = 1.0 / math.sqrt(HD)
    slot_ids = jnp.arange(TILE_SLOTS, dtype=jnp.int32)
    shard = slot_ids // TCAP

    def visit(carry, item):
        m_run, l_run, acc = carry
        relation, src, dst_local, words, counts = item
        live = slot_ids % TCAP < counts[shard]
        dst = (shard * NB_DEV + dst_local).astype(jnp.int32)
        att = rel_att[relation].astype(jnp.float32)
        msg_w = rel_msg[relation].astype(jnp.float32)
        prior = rel_prior[relation] * factor
        qrel = (jnp.einsum('nhe,hde->nhd', query_f, att) * prior[None, :, None]).astype(jnp.bfloat16)
        qrel = qrel.reshape(NBLOCKS, BLOCK, HEADS, HD)
        q_t = qrel[dst].astype(jnp.float32)
        k_t = key_blocks[src].astype(jnp.float32)
        v_t = value_blocks[src].astype(jnp.float32)
        message = jnp.einsum('sjhd,hde->sjhe', v_t, msg_w).astype(jnp.bfloat16)
        scores = jnp.einsum('sihd,sjhd->shij', q_t, k_t)
        edges = unpack(words) & live[:, None, None]
        masked = jnp.where(edges[:, None], scores, NEG)
        block_top = jax.ops.segment_max(masked.max(-1), dst, num_segments=NBLOCKS)
        m_new = jnp.maximum(m_run, block_top)
        weights = jnp.where(edges[:, None], jnp.exp(masked - m_new[dst][..., None]), 0.0)
        rescale = jnp.exp(m_run - m_new)
        l_new = l_run * rescale + jax.ops.segment_sum(weights.sum(-1), dst, num_segments=NBLOCKS)
        pv = jnp.einsum('shij,sjhe->sihe', weights.astype(jnp.bfloat16).astype(jnp.float32), message.astype(jnp.float32))
        acc_new = acc * rescale.transpose(0, 2, 1)[..., None] + jax.ops.segment_sum(pv, dst, num_segments=NBLOCKS)
        return ((m_new, l_new, acc_new), None)
    init = (jnp.full((NBLOCKS, HEADS, BLOCK), NEG, jnp.float32), jnp.zeros((NBLOCKS, HEADS, BLOCK), jnp.float32), jnp.zeros((NBLOCKS, BLOCK, HEADS, HD), jnp.float32))
    (m_run, l_run, acc), _ = lax.scan(visit, init, (rel_perm, tile_src, tile_dst, tile_bits, tile_count))
    totals = l_run.transpose(0, 2, 1).reshape(NODES, HEADS)
    agg = acc.reshape(NODES, D) / jnp.repeat(jnp.maximum(totals, 1.0), HD, axis=1)
    hidden = jax.nn.gelu(agg).astype(jnp.bfloat16)
    mixed = project(hidden, node_type, w_out)
    gate = jax.nn.sigmoid(skip)[node_type][:, None]
    return (gate * mixed + (1.0 - gate) * features.astype(jnp.float32)).astype(jnp.bfloat16)
```

```python
import functools
import math

import jax
import jax.numpy as jnp
from jax import lax
from jax.experimental import pallas as pl
from jax.experimental.pallas import tpu as pltpu
from jax.sharding import PartitionSpec as P

NEG = -1e30
FLOOR = -5e29
LANES = 128
TAIL = 16
GROUP = 4
BF = jnp.bfloat16
F32 = jnp.float32

VMEM = pl.BlockSpec(memory_space=pltpu.VMEM)
SMEM = pl.BlockSpec(memory_space=pltpu.SMEM)
ANY = pl.BlockSpec(memory_space=pl.ANY)


def hits_of(kinds_row, types):
    column = jnp.broadcast_to(kinds_row, (LANES, LANES)).astype(F32).T
    return [jnp.where(column == float(kind), 1.0, 0.0) for kind in range(types)]


def spread(rows, kinds, types):
    wide = rows.shape[1] // LANES
    out = []
    for b in range(rows.shape[0] // LANES):
        block = rows[b * LANES : (b + 1) * LANES]
        parts = []
        for hit in hits_of(kinds[b : b + 1], types):
            parts.append(block * jnp.concatenate([hit.astype(BF)] * wide, axis=1))
        out.append(jnp.concatenate(parts, axis=1))
    return jnp.concatenate(out, axis=0)


def stacked(w_ref):
    types, depth, cols = w_ref.shape
    return w_ref[...].reshape(types * depth, cols)


def kv_body(x_ref, kinds_ref, wk_ref, wv_ref, k_ref, vt_ref):
    types = wk_ref.shape[0]
    cols = wk_ref.shape[2]
    weights = jnp.concatenate([stacked(wk_ref), stacked(wv_ref)], axis=1)
    step = k_ref.shape[0]
    rows = spread(x_ref[...], kinds_ref[0], types)
    both = jnp.dot(rows, weights, preferred_element_type=F32)
    for b in range(step):
        part = both[b * LANES : (b + 1) * LANES]
        k_ref[b] = part[:, :cols].astype(BF)
        vt_ref[b] = part[:, cols:].T.astype(BF)


def q_body(perm_ref, x_ref, kinds_ref, wq_ref, att_ref, msg_ref, qt_ref, attd_ref, msgd_ref, att_s, msg_s, sems):
    types = wq_ref.shape[0]
    positions = attd_ref.shape[0]
    heads, hd = att_ref.shape[1], att_ref.shape[2]
    step = qt_ref.shape[0]

    def copies(p):
        r = perm_ref[p]
        return (
            pltpu.make_async_copy(att_ref.at[r], att_s.at[p], sems.at[0, p]),
            pltpu.make_async_copy(msg_ref.at[r], msg_s.at[p], sems.at[1, p]),
        )

    @pl.when(pl.program_id(0) == 0)
    def _():
        for p in range(positions):
            for copy in copies(p):
                copy.start()

    rows = spread(x_ref[...], kinds_ref[0], types)
    query = jnp.dot(rows, stacked(wq_ref), preferred_element_type=F32)
    for b in range(step):
        qt_ref[b] = query[b * LANES : (b + 1) * LANES].T.astype(BF)

    @pl.when(pl.program_id(0) == pl.num_programs(0) - 1)
    def _():
        for p in range(positions):
            for copy in copies(p):
                copy.wait()
        for p in range(positions):
            for h in range(heads):
                pads = [jnp.zeros((hd, hd), F32)] * heads
                lanes = list(pads)
                lanes[h] = att_s[p, h].astype(F32)
                attd_ref[p, h * hd : (h + 1) * hd, :] = jnp.concatenate(lanes, axis=1).astype(BF)
                lanes = list(pads)
                lanes[h] = msg_s[p, h].astype(F32).T
                msgd_ref[p, h * hd : (h + 1) * hd, :] = jnp.concatenate(lanes, axis=1).astype(BF)


def tiles_body(
    heads, tcap, n_rel, first, last, list_ref, ends_ref, prior_ref, bits_ref, qt_ref, k_ref, vt_ref, attd_ref, msgd_ref, *refs
):
    if first == 0:
        start = 0
    else:
        start = ends_ref[first - 1]
        old_m, old_l, old_a, *refs = refs
    stop = ends_ref[first]
    if last:
        send_ref, m_ref, l_ref, a_ref = refs
    else:
        m_ref, l_ref, a_ref = refs
    cols = qt_ref.shape[1]
    hd = cols // heads
    wide = heads * LANES
    if first == 0:
        m_ref[...] = jnp.full(m_ref.shape, FLOOR, F32)
        l_ref[...] = jnp.zeros(l_ref.shape, F32)
        a_ref[...] = jnp.zeros(a_ref.shape, F32)
    else:
        m_ref[...] = old_m[...]
        l_ref[...] = old_l[...]
        a_ref[...] = old_a[...]
    shift = 31 - lax.broadcasted_iota(jnp.int32, (32, LANES), 0)

    def tile(index):
        code = list_ref[jnp.minimum(index, stop - 1)]
        slot = code & 0xFFF
        src = (code >> 12) & 0xFFF
        dst = code >> 24
        position = lax.div(slot, tcap)
        words = jnp.where(index < stop, bits_ref[slot], 0)
        qrel = jnp.dot(attd_ref[position], qt_ref[dst], preferred_element_type=F32)
        diag = []
        for h in range(heads):
            piece = (qrel[h * hd : (h + 1) * hd] * prior_ref[position * heads + h]).astype(BF)
            row = [jnp.zeros((hd, LANES), BF)] * heads
            row[h] = piece
            diag.append(jnp.concatenate(row, axis=1))
        scores = jnp.dot(k_ref[src], jnp.concatenate(diag, axis=0), preferred_element_type=F32)
        message = jnp.dot(msgd_ref[position], vt_ref[src], preferred_element_type=F32).astype(BF)
        parts = []
        for w in range(words.shape[0]):
            edge = (jnp.broadcast_to(words[w : w + 1], (32, LANES)) << shift) < 0
            for_heads = jnp.concatenate([edge] * heads, axis=1)
            parts.append(jnp.where(for_heads, scores[w * 32 : (w + 1) * 32], NEG))
        masked = jnp.concatenate(parts, axis=0)
        top = jnp.maximum(jnp.max(masked, axis=0, keepdims=True), FLOOR)
        weights = jnp.exp(masked - top)
        total = jnp.sum(weights, axis=0, keepdims=True)
        rounded = weights.astype(BF)
        sums = []
        for h in range(heads):
            sums.append(
                jnp.dot(
                    message[h * hd : (h + 1) * hd],
                    rounded[:, h * LANES : (h + 1) * LANES],
                    preferred_element_type=F32,
                )
            )
        return dst, top, total, sums

    def visit(turn, carry):
        done = [tile(start + turn * GROUP + g) for g in range(GROUP)]
        for dst, top, total, sums in done:
            m_old = m_ref[dst]
            m_new = jnp.maximum(m_old, top)
            keep = jnp.exp(m_old - m_new)
            take = jnp.exp(top - m_new)
            m_ref[dst] = m_new
            l_ref[dst] = l_ref[dst] * keep + total * take
            for h in range(heads):
                lanes = slice(h * LANES, (h + 1) * LANES)
                rows = slice(h * hd, (h + 1) * hd)
                a_ref[dst, rows, :] = a_ref[dst, rows, :] * keep[:, lanes] + sums[h] * take[:, lanes]
        return carry

    lax.fori_loop(0, lax.div(stop - start + GROUP - 1, GROUP), visit, 0)

    if last:
        blocks = a_ref.shape[0]
        n_head = blocks // n_rel
        for b in range(blocks):
            spot = (b % n_rel) * n_head + b // n_rel
            send_ref[spot, :cols, :] = a_ref[b].astype(BF)
            rows = []
            for value, count in ((m_ref[b], 3), (l_ref[b], 3)):
                rest = value
                for _ in range(count):
                    piece = rest.astype(BF).astype(F32)
                    rest = rest - piece
                    rows += [piece[:, h * LANES : (h + 1) * LANES] for h in range(heads)]
            rows.append(jnp.zeros((TAIL - len(rows), LANES), F32))
            send_ref[spot, cols:, :] = jnp.concatenate(rows, axis=0).astype(BF)


def finish_body(heads, n_rel, n_head, me_ref, skip_ref, got_ref, x_ref, kinds_ref, *refs):
    w_refs, out_ref = refs[:-1], refs[-1]
    cols = got_ref.shape[1] - TAIL
    hd = cols // heads
    types = w_refs[0].shape[0]
    hits = hits_of(kinds_ref[...], types)
    hidden = []
    for s in range(n_head):
        h_from = lax.rem(me_ref[0] + n_head - s, n_head)
        accs, tops, totals = [], [], []
        for z in range(n_rel):
            spot = z * n_head + h_from
            accs.append(got_ref[spot, :cols, :])
            tail = got_ref[spot, cols:, :].astype(F32)
            m = tail[0:heads] + tail[heads : 2 * heads] + tail[2 * heads : 3 * heads]
            tail = tail[3 * heads :]
            tops.append(m)
            totals.append(tail[0:heads] + tail[heads : 2 * heads] + tail[2 * heads : 3 * heads])
        top = functools.reduce(jnp.maximum, tops)
        scales = [jnp.exp(m - top) for m in tops]
        total = functools.reduce(jnp.add, [l * e for l, e in zip(totals, scales)])
        inverse = 1.0 / jnp.maximum(total, 1.0)
        rows = []
        for h in range(heads):
            acc = functools.reduce(
                jnp.add,
                [a[h * hd : (h + 1) * hd].astype(F32) * e[h : h + 1] for a, e in zip(accs, scales)],
            )
            rows.append(jax.nn.gelu(acc * inverse[h : h + 1]))
        hidden.append(jnp.concatenate(rows, axis=0).T.astype(BF))
    mixed = None
    for s in range(n_head):
        w = w_refs[s][...].reshape(types * cols, -1)
        spread_rows = jnp.concatenate([hidden[s] * hit.astype(BF) for hit in hits], axis=1)
        part = jnp.dot(spread_rows, w, preferred_element_type=F32)
        mixed = part if mixed is None else mixed + part
    gate = jnp.zeros((LANES, LANES), F32)
    for kind in range(types):
        gate = gate + hits[kind] * jax.nn.sigmoid(jnp.full((LANES, LANES), skip_ref[kind], F32))
    gate = jnp.concatenate([gate] * (mixed.shape[1] // LANES), axis=1)
    out_ref[...] = (gate * mixed + (1.0 - gate) * x_ref[...].astype(F32)).astype(BF)


def shifted(n, s):
    return [(i, (i + s) % n) for i in range(n)]


def listed(tile_src, tile_dst, tile_count, blocks, me, n_node):
    positions, tcap = tile_src.shape
    slots = positions * tcap
    src = tile_src.reshape(slots)
    dst = tile_dst.reshape(slots)
    ids = jnp.arange(slots, dtype=jnp.int32)
    live = (jnp.arange(tcap, dtype=jnp.int32)[None, :] < tile_count).reshape(slots)
    away = (me - src // blocks) % n_node
    near = live & (away == 0)
    far = live & (away != 0)
    place = src % blocks + jnp.maximum(away - 1, 0) * blocks
    code = ids | (place << 12) | (dst << 24)
    n_near = jnp.sum(near.astype(jnp.int32))
    n_live = jnp.sum(live.astype(jnp.int32))
    before = ids[None, :] < ids[:, None]
    near_rank = jnp.sum((before & near[None, :]).astype(jnp.int32), axis=1)
    far_rank = jnp.sum((before & far[None, :]).astype(jnp.int32), axis=1)
    rank = jnp.where(near, near_rank, jnp.where(far, n_near + far_rank, -1))
    order = jnp.sum(jnp.where(rank[None, :] == ids[:, None], code[None, :], 0), axis=1)
    return order, jnp.stack([n_near, n_live])


def per_device(
    features,
    node_type,
    w_query,
    w_key,
    w_value,
    rel_att,
    rel_msg,
    rel_prior,
    w_out,
    skip,
    rel_perm,
    tile_src,
    tile_dst,
    tile_bits,
    tile_count,
):
    node_rows, depth = features.shape
    n_rel = lax.axis_size("rel")
    n_node = lax.axis_size("node")
    n_head = lax.axis_size("head")
    heads = rel_prior.shape[1]
    types, _, cols = w_query.shape
    hd = cols // heads
    positions, tcap, block, words = tile_bits.shape
    blocks = node_rows // block
    slots = positions * tcap
    kinds = node_type.reshape(blocks, block)

    w_parts = [w_out] + [lax.ppermute(w_out, "head", shifted(n_head, s)) for s in range(1, n_head)]

    step = math.gcd(4, blocks)
    x_spec = pl.BlockSpec((step * block, depth), lambda i: (i, 0))
    kinds_spec = pl.BlockSpec((1, step, block), lambda i: (i, 0, 0))
    w_spec = pl.BlockSpec((types, depth, cols), lambda i: (0, 0, 0))
    b_spec = pl.BlockSpec((step, block, cols), lambda i: (i, 0, 0))
    bt_spec = pl.BlockSpec((step, cols, block), lambda i: (i, 0, 0))
    kinds_in = kinds.reshape(blocks // step, step, block)
    keys, values_t = pl.pallas_call(
        kv_body,
        grid=(blocks // step,),
        in_specs=[x_spec, kinds_spec, w_spec, w_spec],
        out_specs=[b_spec, bt_spec],
        out_shape=[
            jax.ShapeDtypeStruct((blocks, block, cols), BF),
            jax.ShapeDtypeStruct((blocks, cols, block), BF),
        ],
        name="keys_values",
    )(features, kinds_in, w_key, w_value)

    far_keys = [lax.ppermute(keys, "node", shifted(n_node, s)) for s in range(1, n_node)]
    far_values = [lax.ppermute(values_t, "node", shifted(n_node, s)) for s in range(1, n_node)]

    d_spec = pl.BlockSpec((positions, cols, cols), lambda i, perm: (0, 0, 0))
    queries_t, att_d, msg_d = pl.pallas_call(
        q_body,
        grid_spec=pltpu.PrefetchScalarGridSpec(
            num_scalar_prefetch=1,
            grid=(blocks // step,),
            in_specs=[
                pl.BlockSpec((step * block, depth), lambda i, perm: (i, 0)),
                pl.BlockSpec((1, step, block), lambda i, perm: (i, 0, 0)),
                pl.BlockSpec((types, depth, cols), lambda i, perm: (0, 0, 0)),
                ANY,
                ANY,
            ],
            out_specs=[pl.BlockSpec((step, cols, block), lambda i, perm: (i, 0, 0)), d_spec, d_spec],
            scratch_shapes=[
                pltpu.VMEM((positions, heads, hd, hd), BF),
                pltpu.VMEM((positions, heads, hd, hd), BF),
                pltpu.SemaphoreType.DMA((2, positions)),
            ],
        ),
        out_shape=[
            jax.ShapeDtypeStruct((blocks, cols, block), BF),
            jax.ShapeDtypeStruct((positions, cols, cols), BF),
            jax.ShapeDtypeStruct((positions, cols, cols), BF),
        ],
        name="queries",
    )(rel_perm, features, kinds_in, w_query, rel_att, rel_msg)

    order, ends = listed(tile_src, tile_dst, tile_count, blocks, lax.axis_index("node"), n_node)
    prior = (rel_prior[rel_perm] * (1.0 / math.sqrt(hd))).reshape(positions * heads)
    bits = tile_bits.transpose(0, 1, 3, 2).reshape(slots, words, block)
    state_shapes = [
        jax.ShapeDtypeStruct((blocks, 1, heads * block), F32),
        jax.ShapeDtypeStruct((blocks, 1, heads * block), F32),
        jax.ShapeDtypeStruct((blocks, cols, block), F32),
    ]
    state = pl.pallas_call(
        functools.partial(tiles_body, heads, tcap, n_rel, 0, False),
        in_specs=[SMEM, SMEM, SMEM] + [VMEM] * 6,
        out_specs=[VMEM] * 3,
        out_shape=state_shapes,
        name="near_tiles",
    )(order, ends, prior, bits, queries_t, keys, values_t, att_d, msg_d)

    def joined(arrays):
        return arrays[0] if len(arrays) == 1 else jnp.concatenate(arrays, axis=0)

    send = pl.pallas_call(
        functools.partial(tiles_body, heads, tcap, n_rel, 1, True),
        in_specs=[SMEM, SMEM, SMEM] + [VMEM] * 9,
        out_specs=VMEM,
        out_shape=jax.ShapeDtypeStruct((blocks, cols + TAIL, block), BF),
        scratch_shapes=[pltpu.VMEM(s.shape, s.dtype) for s in state_shapes],
        name="far_tiles",
    )(order, ends, prior, bits, queries_t, joined(far_keys), joined(far_values), att_d, msg_d, *state)

    got = lax.all_to_all(send, ("rel", "head"), 0, 0, tiled=True)

    spot = lax.axis_index("head") * n_rel + lax.axis_index("rel")
    own_rows = lax.dynamic_slice_in_dim(features, spot * block, block, 0)
    own_kinds = lax.dynamic_slice_in_dim(kinds, spot, 1, 0)
    finished = pl.pallas_call(
        functools.partial(finish_body, heads, n_rel, n_head),
        in_specs=[SMEM, SMEM] + [VMEM] * (3 + n_head),
        out_specs=VMEM,
        out_shape=jax.ShapeDtypeStruct((block, depth), BF),
        name="finish",
    )(lax.axis_index("head").reshape(1), skip, got, own_rows, own_kinds, *w_parts)
    return lax.all_gather(finished, "rel", axis=0, tiled=True)


def solution(mesh):
    in_specs = (
        P("node", None),
        P("node"),
        P(None, None, "head"),
        P(None, None, "head"),
        P(None, None, "head"),
        P(None, "head", None, None),
        P(None, "head", None, None),
        P(None, "head"),
        P(None, "head", None),
        P(),
        P("rel"),
        P("rel", "node"),
        P("rel", "node"),
        P("rel", "node", None, None),
        P("rel", "node"),
    )
    out_specs = P(("node", "head"), None)
    return jax.shard_map(
        per_device, mesh=mesh, in_specs=in_specs, out_specs=out_specs, check_vma=False
    )
```

```python
import functools
import math

import jax
import jax.numpy as jnp
from jax import lax
from jax.experimental import pallas as pl
from jax.experimental.pallas import tpu as pltpu
from jax.sharding import PartitionSpec as P


NEG = -1e30
FLOOR = -5e29
LANES = 128
TAIL = 16
GROUP = 4
BF = jnp.bfloat16
F32 = jnp.float32

VMEM = pl.BlockSpec(memory_space=pltpu.VMEM)
SMEM = pl.BlockSpec(memory_space=pltpu.SMEM)
ANY = pl.BlockSpec(memory_space=pl.ANY)


def hits_of(kinds_row, types):
    column = jnp.broadcast_to(kinds_row, (LANES, LANES)).astype(F32).T
    return [jnp.where(column == float(kind), 1.0, 0.0) for kind in range(types)]


def spread(rows, kinds, types):
    wide = rows.shape[1] // LANES
    out = []
    for b in range(rows.shape[0] // LANES):
        block = rows[b * LANES : (b + 1) * LANES]
        parts = []
        for hit in hits_of(kinds[b : b + 1], types):
            parts.append(block * jnp.concatenate([hit.astype(BF)] * wide, axis=1))
        out.append(jnp.concatenate(parts, axis=1))
    return jnp.concatenate(out, axis=0)


def stacked(w_ref):
    types, depth, cols = w_ref.shape
    return w_ref[...].reshape(types * depth, cols)


def kv_body(x_ref, kinds_ref, wk_ref, wv_ref, k_ref, vt_ref):
    types = wk_ref.shape[0]
    cols = wk_ref.shape[2]
    weights = jnp.concatenate([stacked(wk_ref), stacked(wv_ref)], axis=1)
    step = k_ref.shape[0]
    rows = spread(x_ref[...], kinds_ref[0], types)
    both = jnp.dot(rows, weights, preferred_element_type=F32)
    for b in range(step):
        part = both[b * LANES : (b + 1) * LANES]
        k_ref[b] = part[:, :cols].astype(BF)
        vt_ref[b] = part[:, cols:].T.astype(BF)


def q_body(perm_ref, x_ref, kinds_ref, wq_ref, att_ref, msg_ref, qt_ref, attd_ref, msgd_ref, att_s, msg_s, sems):
    types = wq_ref.shape[0]
    positions = attd_ref.shape[0]
    heads, hd = att_ref.shape[1], att_ref.shape[2]
    step = qt_ref.shape[0]

    def copies(p):
        r = perm_ref[p]
        return (
            pltpu.make_async_copy(att_ref.at[r], att_s.at[p], sems.at[0, p]),
            pltpu.make_async_copy(msg_ref.at[r], msg_s.at[p], sems.at[1, p]),
        )

    @pl.when(pl.program_id(0) == 0)
    def _():
        for p in range(positions):
            for copy in copies(p):
                copy.start()

    rows = spread(x_ref[...], kinds_ref[0], types)
    query = jnp.dot(rows, stacked(wq_ref), preferred_element_type=F32)
    for b in range(step):
        qt_ref[b] = query[b * LANES : (b + 1) * LANES].T.astype(BF)

    @pl.when(pl.program_id(0) == pl.num_programs(0) - 1)
    def _():
        for p in range(positions):
            for copy in copies(p):
                copy.wait()
        for p in range(positions):
            for h in range(heads):
                pads = [jnp.zeros((hd, hd), F32)] * heads
                lanes = list(pads)
                lanes[h] = att_s[p, h].astype(F32)
                attd_ref[p, h * hd : (h + 1) * hd, :] = jnp.concatenate(lanes, axis=1).astype(BF)
                lanes = list(pads)
                lanes[h] = msg_s[p, h].astype(F32).T
                msgd_ref[p, h * hd : (h + 1) * hd, :] = jnp.concatenate(lanes, axis=1).astype(BF)


def tiles_body(
    heads, tcap, n_rel, first, last, list_ref, ends_ref, prior_ref, bits_ref, qt_ref, k_ref, vt_ref, attd_ref, msgd_ref, *refs
):
    if first == 0:
        start = 0
    else:
        start = ends_ref[first - 1]
        old_m, old_l, old_a, *refs = refs
    stop = ends_ref[first]
    *refs, q_s, w_s, v_s, t_s = refs
    if last:
        send_ref, m_ref, l_ref, a_ref = refs
    else:
        m_ref, l_ref, a_ref = refs
    cols = qt_ref.shape[1]
    hd = cols // heads
    if first == 0:
        m_ref[...] = jnp.full(m_ref.shape, FLOOR, F32)
        l_ref[...] = jnp.zeros(l_ref.shape, F32)
        a_ref[...] = jnp.zeros(a_ref.shape, F32)
    else:
        m_ref[...] = old_m[...]
        l_ref[...] = old_l[...]
        a_ref[...] = old_a[...]
    q_s[...] = jnp.zeros(q_s.shape, BF)
    w_s[...] = jnp.zeros(w_s.shape, BF)
    v_s[...] = jnp.zeros(v_s.shape, BF)
    t_s[0] = jnp.full(t_s.shape[1:], FLOOR, F32)
    t_s[1] = jnp.zeros(t_s.shape[1:], F32)
    shift = 31 - lax.broadcasted_iota(jnp.int32, (32, LANES), 0)

    def read(index):
        code = list_ref[jnp.clip(index, start, stop - 1)]
        slot = code & 0xFFF
        return slot, (code >> 12) & 0xFFF, code >> 24, lax.div(slot, tcap)

    def visit(turn, carry):
        base = start + turn * GROUP
        sums, scores, messages, queries = [], [], [], []
        for g in range(GROUP):
            sums.append(
                [
                    jnp.dot(
                        v_s[g, h * hd : (h + 1) * hd, :],
                        w_s[g, :, h * LANES : (h + 1) * LANES],
                        preferred_element_type=F32,
                    )
                    for h in range(heads)
                ]
            )
        for g in range(GROUP):
            slot, src, dst, position = read(base - GROUP + g)
            scores.append(jnp.dot(k_ref[src], q_s[g], preferred_element_type=F32))
            messages.append(jnp.dot(msgd_ref[position], vt_ref[src], preferred_element_type=F32))
        for g in range(GROUP):
            slot, src, dst, position = read(base + g)
            queries.append(jnp.dot(attd_ref[position], qt_ref[dst], preferred_element_type=F32))
        for g in range(GROUP):
            slot, src, dst, position = read(base - 2 * GROUP + g)
            top, total = t_s[0, g], t_s[1, g]
            m_old = m_ref[dst]
            m_new = jnp.maximum(m_old, top)
            keep = jnp.exp(m_old - m_new)
            take = jnp.exp(top - m_new)
            m_ref[dst] = m_new
            l_ref[dst] = l_ref[dst] * keep + total * take
            for h in range(heads):
                lanes = slice(h * LANES, (h + 1) * LANES)
                rows = slice(h * hd, (h + 1) * hd)
                a_ref[dst, rows, :] = a_ref[dst, rows, :] * keep[:, lanes] + sums[g][h] * take[:, lanes]
        for g in range(GROUP):
            index = base - GROUP + g
            slot, src, dst, position = read(index)
            valid = jnp.logical_and(index >= start, index < stop)
            words = jnp.where(valid, bits_ref[slot], 0)
            parts = []
            for w in range(words.shape[0]):
                edge = (jnp.broadcast_to(words[w : w + 1], (32, LANES)) << shift) < 0
                for_heads = jnp.concatenate([edge] * heads, axis=1)
                parts.append(jnp.where(for_heads, scores[g][w * 32 : (w + 1) * 32], NEG))
            masked = jnp.concatenate(parts, axis=0)
            top = jnp.maximum(jnp.max(masked, axis=0, keepdims=True), FLOOR)
            weights = jnp.exp(masked - top)
            t_s[0, g] = top
            t_s[1, g] = jnp.sum(weights, axis=0, keepdims=True)
            w_s[g] = weights.astype(BF)
            v_s[g] = messages[g].astype(BF)
        for g in range(GROUP):
            slot, src, dst, position = read(base + g)
            for h in range(heads):
                rows = slice(h * hd, (h + 1) * hd)
                piece = queries[g][rows] * prior_ref[position * heads + h]
                q_s[g, rows, h * LANES : (h + 1) * LANES] = piece.astype(BF)
        return carry

    count = stop - start
    lax.fori_loop(0, jnp.where(count > 0, lax.div(count + GROUP - 1, GROUP) + 2, 0), visit, 0)

    if last:
        blocks = a_ref.shape[0]
        n_head = blocks // n_rel
        for b in range(blocks):
            spot = (b % n_rel) * n_head + b // n_rel
            send_ref[spot, :cols, :] = a_ref[b].astype(BF)
            rows = []
            for value, count in ((m_ref[b], 3), (l_ref[b], 3)):
                rest = value
                for _ in range(count):
                    piece = rest.astype(BF).astype(F32)
                    rest = rest - piece
                    rows += [piece[:, h * LANES : (h + 1) * LANES] for h in range(heads)]
            rows.append(jnp.zeros((TAIL - len(rows), LANES), F32))
            send_ref[spot, cols:, :] = jnp.concatenate(rows, axis=0).astype(BF)


def finish_body(heads, n_rel, n_head, me_ref, skip_ref, got_ref, x_ref, kinds_ref, *refs):
    w_refs, out_ref = refs[:-1], refs[-1]
    cols = got_ref.shape[1] - TAIL
    hd = cols // heads
    types = w_refs[0].shape[0]
    hits = hits_of(kinds_ref[...], types)
    hidden = []
    for s in range(n_head):
        h_from = lax.rem(me_ref[0] + n_head - s, n_head)
        accs, tops, totals = [], [], []
        for z in range(n_rel):
            spot = z * n_head + h_from
            accs.append(got_ref[spot, :cols, :])
            tail = got_ref[spot, cols:, :].astype(F32)
            m = tail[0:heads] + tail[heads : 2 * heads] + tail[2 * heads : 3 * heads]
            tail = tail[3 * heads :]
            tops.append(m)
            totals.append(tail[0:heads] + tail[heads : 2 * heads] + tail[2 * heads : 3 * heads])
        top = functools.reduce(jnp.maximum, tops)
        scales = [jnp.exp(m - top) for m in tops]
        total = functools.reduce(jnp.add, [l * e for l, e in zip(totals, scales)])
        inverse = 1.0 / jnp.maximum(total, 1.0)
        rows = []
        for h in range(heads):
            acc = functools.reduce(
                jnp.add,
                [a[h * hd : (h + 1) * hd].astype(F32) * e[h : h + 1] for a, e in zip(accs, scales)],
            )
            rows.append(jax.nn.gelu(acc * inverse[h : h + 1]))
        hidden.append(jnp.concatenate(rows, axis=0).T.astype(BF))
    mixed = None
    for s in range(n_head):
        w = w_refs[s][...].reshape(types * cols, -1)
        spread_rows = jnp.concatenate([hidden[s] * hit.astype(BF) for hit in hits], axis=1)
        part = jnp.dot(spread_rows, w, preferred_element_type=F32)
        mixed = part if mixed is None else mixed + part
    gate = jnp.zeros((LANES, LANES), F32)
    for kind in range(types):
        gate = gate + hits[kind] * jax.nn.sigmoid(jnp.full((LANES, LANES), skip_ref[kind], F32))
    gate = jnp.concatenate([gate] * (mixed.shape[1] // LANES), axis=1)
    out_ref[...] = (gate * mixed + (1.0 - gate) * x_ref[...].astype(F32)).astype(BF)


def shifted(n, s):
    return [(i, (i + s) % n) for i in range(n)]


def listed(tile_src, tile_dst, tile_count, blocks, me, n_node):
    positions, tcap = tile_src.shape
    slots = positions * tcap
    src = tile_src.reshape(slots)
    dst = tile_dst.reshape(slots)
    ids = jnp.arange(slots, dtype=jnp.int32)
    live = (jnp.arange(tcap, dtype=jnp.int32)[None, :] < tile_count).reshape(slots)
    away = (me - src // blocks) % n_node
    near = live & (away == 0)
    far = live & (away != 0)
    place = src % blocks + jnp.maximum(away - 1, 0) * blocks
    code = ids | (place << 12) | (dst << 24)
    n_near = jnp.sum(near.astype(jnp.int32))
    n_live = jnp.sum(live.astype(jnp.int32))
    before = ids[None, :] < ids[:, None]
    near_rank = jnp.sum((before & near[None, :]).astype(jnp.int32), axis=1)
    far_rank = jnp.sum((before & far[None, :]).astype(jnp.int32), axis=1)
    rank = jnp.where(near, near_rank, jnp.where(far, n_near + far_rank, -1))
    order = jnp.sum(jnp.where(rank[None, :] == ids[:, None], code[None, :], 0), axis=1)
    return order, jnp.stack([n_near, n_live])


def layer(
    features,
    node_type,
    w_query,
    w_key,
    w_value,
    rel_att,
    rel_msg,
    rel_prior,
    w_out,
    skip,
    rel_perm,
    tile_src,
    tile_dst,
    tile_bits,
    tile_count,
):
    node_rows, depth = features.shape
    n_rel = lax.axis_size("rel")
    n_node = lax.axis_size("node")
    n_head = lax.axis_size("head")
    heads = rel_prior.shape[1]
    types, _, cols = w_query.shape
    hd = cols // heads
    positions, tcap, block, words = tile_bits.shape
    blocks = node_rows // block
    slots = positions * tcap
    kinds = node_type.reshape(blocks, block)

    w_parts = [w_out] + [lax.ppermute(w_out, "head", shifted(n_head, s)) for s in range(1, n_head)]

    step = math.gcd(4, blocks)
    x_spec = pl.BlockSpec((step * block, depth), lambda i: (i, 0))
    kinds_spec = pl.BlockSpec((1, step, block), lambda i: (i, 0, 0))
    w_spec = pl.BlockSpec((types, depth, cols), lambda i: (0, 0, 0))
    b_spec = pl.BlockSpec((step, block, cols), lambda i: (i, 0, 0))
    bt_spec = pl.BlockSpec((step, cols, block), lambda i: (i, 0, 0))
    kinds_in = kinds.reshape(blocks // step, step, block)
    keys, values_t = pl.pallas_call(
        kv_body,
        grid=(blocks // step,),
        in_specs=[x_spec, kinds_spec, w_spec, w_spec],
        out_specs=[b_spec, bt_spec],
        out_shape=[
            jax.ShapeDtypeStruct((blocks, block, cols), BF),
            jax.ShapeDtypeStruct((blocks, cols, block), BF),
        ],
        name="keys_values",
    )(features, kinds_in, w_key, w_value)

    far_keys = [lax.ppermute(keys, "node", shifted(n_node, s)) for s in range(1, n_node)]
    far_values = [lax.ppermute(values_t, "node", shifted(n_node, s)) for s in range(1, n_node)]

    d_spec = pl.BlockSpec((positions, cols, cols), lambda i, perm: (0, 0, 0))
    queries_t, att_d, msg_d = pl.pallas_call(
        q_body,
        grid_spec=pltpu.PrefetchScalarGridSpec(
            num_scalar_prefetch=1,
            grid=(blocks // step,),
            in_specs=[
                pl.BlockSpec((step * block, depth), lambda i, perm: (i, 0)),
                pl.BlockSpec((1, step, block), lambda i, perm: (i, 0, 0)),
                pl.BlockSpec((types, depth, cols), lambda i, perm: (0, 0, 0)),
                ANY,
                ANY,
            ],
            out_specs=[pl.BlockSpec((step, cols, block), lambda i, perm: (i, 0, 0)), d_spec, d_spec],
            scratch_shapes=[
                pltpu.VMEM((positions, heads, hd, hd), BF),
                pltpu.VMEM((positions, heads, hd, hd), BF),
                pltpu.SemaphoreType.DMA((2, positions)),
            ],
        ),
        out_shape=[
            jax.ShapeDtypeStruct((blocks, cols, block), BF),
            jax.ShapeDtypeStruct((positions, cols, cols), BF),
            jax.ShapeDtypeStruct((positions, cols, cols), BF),
        ],
        name="queries",
    )(rel_perm, features, kinds_in, w_query, rel_att, rel_msg)

    order, ends = listed(tile_src, tile_dst, tile_count, blocks, lax.axis_index("node"), n_node)
    prior = (rel_prior[rel_perm] * (1.0 / math.sqrt(hd))).reshape(positions * heads)
    bits = tile_bits.transpose(0, 1, 3, 2).reshape(slots, words, block)
    state_shapes = [
        jax.ShapeDtypeStruct((blocks, 1, heads * block), F32),
        jax.ShapeDtypeStruct((blocks, 1, heads * block), F32),
        jax.ShapeDtypeStruct((blocks, cols, block), F32),
    ]
    stage = [
        pltpu.VMEM((GROUP, cols, heads * block), BF),
        pltpu.VMEM((GROUP, block, heads * block), BF),
        pltpu.VMEM((GROUP, cols, block), BF),
        pltpu.VMEM((2, GROUP, 1, heads * block), F32),
    ]
    state = pl.pallas_call(
        functools.partial(tiles_body, heads, tcap, n_rel, 0, False),
        in_specs=[SMEM, SMEM, SMEM] + [VMEM] * 6,
        out_specs=[VMEM] * 3,
        out_shape=state_shapes,
        scratch_shapes=stage,
        name="near_tiles",
    )(order, ends, prior, bits, queries_t, keys, values_t, att_d, msg_d)

    def joined(arrays):
        return arrays[0] if len(arrays) == 1 else jnp.concatenate(arrays, axis=0)

    send = pl.pallas_call(
        functools.partial(tiles_body, heads, tcap, n_rel, 1, True),
        in_specs=[SMEM, SMEM, SMEM] + [VMEM] * 9,
        out_specs=VMEM,
        out_shape=jax.ShapeDtypeStruct((blocks, cols + TAIL, block), BF),
        scratch_shapes=[pltpu.VMEM(s.shape, s.dtype) for s in state_shapes] + stage,
        name="far_tiles",
    )(order, ends, prior, bits, queries_t, joined(far_keys), joined(far_values), att_d, msg_d, *state)

    got = lax.all_to_all(send, ("rel", "head"), 0, 0, tiled=True)

    spot = lax.axis_index("head") * n_rel + lax.axis_index("rel")
    own_rows = lax.dynamic_slice_in_dim(features, spot * block, block, 0)
    own_kinds = lax.dynamic_slice_in_dim(kinds, spot, 1, 0)
    finished = pl.pallas_call(
        functools.partial(finish_body, heads, n_rel, n_head),
        in_specs=[SMEM, SMEM] + [VMEM] * (3 + n_head),
        out_specs=VMEM,
        out_shape=jax.ShapeDtypeStruct((block, depth), BF),
        name="finish",
    )(lax.axis_index("head").reshape(1), skip, got, own_rows, own_kinds, *w_parts)
    return lax.all_gather(finished, "rel", axis=0, tiled=True)


def solution(mesh):
    in_specs = (
        P("node", None),
        P("node"),
        P(None, None, "head"),
        P(None, None, "head"),
        P(None, None, "head"),
        P(None, "head", None, None),
        P(None, "head", None, None),
        P(None, "head"),
        P(None, "head", None),
        P(),
        P("rel"),
        P("rel", "node"),
        P("rel", "node"),
        P("rel", "node", None, None),
        P("rel", "node"),
    )
    out_specs = P(("node", "head"), None)
    return jax.shard_map(layer, mesh=mesh, in_specs=in_specs, out_specs=out_specs, check_vma=False)
```

```python
import functools
import math

import jax
import jax.numpy as jnp
from jax import lax
from jax.experimental import pallas as pl
from jax.experimental.pallas import tpu as pltpu
from jax.sharding import PartitionSpec as P


NEG = -1e30
FLOOR = -5e29
LANES = 128
TAIL = 16
GROUP = 4
BF = jnp.bfloat16
F32 = jnp.float32

VMEM = pl.BlockSpec(memory_space=pltpu.VMEM)
SMEM = pl.BlockSpec(memory_space=pltpu.SMEM)
ANY = pl.BlockSpec(memory_space=pl.ANY)
SMALL = pltpu.CompilerParams(vmem_limit_bytes=16 << 20)


def hits_of(kinds_row, types):
    column = jnp.broadcast_to(kinds_row, (LANES, LANES)).astype(F32).T
    return [jnp.where(column == float(kind), 1.0, 0.0) for kind in range(types)]


def spread(rows, kinds, types):
    wide = rows.shape[1] // LANES
    out = []
    for b in range(rows.shape[0] // LANES):
        block = rows[b * LANES : (b + 1) * LANES]
        parts = []
        for hit in hits_of(kinds[b : b + 1], types):
            parts.append(block * jnp.concatenate([hit.astype(BF)] * wide, axis=1))
        out.append(jnp.concatenate(parts, axis=1))
    return jnp.concatenate(out, axis=0)


def stacked(w_ref):
    types, depth, cols = w_ref.shape
    return w_ref[...].reshape(types * depth, cols)


def kv_body(x_ref, kinds_ref, wk_ref, wv_ref, k_ref, vt_ref):
    types = wk_ref.shape[0]
    cols = wk_ref.shape[2]
    weights = jnp.concatenate([stacked(wk_ref), stacked(wv_ref)], axis=1)
    step = k_ref.shape[0]
    rows = spread(x_ref[...], kinds_ref[0], types)
    both = jnp.dot(rows, weights, preferred_element_type=F32)
    for b in range(step):
        part = both[b * LANES : (b + 1) * LANES]
        k_ref[b] = part[:, :cols].astype(BF)
        vt_ref[b] = part[:, cols:].T.astype(BF)


def q_body(perm_ref, x_ref, kinds_ref, wq_ref, att_ref, msg_ref, qt_ref, atts_ref, msgt_ref, msg_s, sems):
    types = wq_ref.shape[0]
    positions, heads = msg_s.shape[:2]
    step = qt_ref.shape[0]

    def copies(p):
        r = perm_ref[p]
        return (
            pltpu.make_async_copy(att_ref.at[r], atts_ref.at[p], sems.at[0, p]),
            pltpu.make_async_copy(msg_ref.at[r], msg_s.at[p], sems.at[1, p]),
        )

    @pl.when(pl.program_id(0) == 0)
    def _():
        for p in range(positions):
            for copy in copies(p):
                copy.start()

    rows = spread(x_ref[...], kinds_ref[0], types)
    query = jnp.dot(rows, stacked(wq_ref), preferred_element_type=F32)
    for b in range(step):
        qt_ref[b] = query[b * LANES : (b + 1) * LANES].T.astype(BF)

    @pl.when(pl.program_id(0) == pl.num_programs(0) - 1)
    def _():
        for p in range(positions):
            for copy in copies(p):
                copy.wait()
        for p in range(positions):
            for h in range(heads):
                msgt_ref[p, h] = msg_s[p, h].astype(F32).T.astype(BF)


def split(x, n):
    if n & (n - 1) == 0:
        return x >> (n.bit_length() - 1), x & (n - 1)
    return lax.div(x, n), lax.rem(x, n)


def build_lists(n_node, blocks, me, src_ref, dst_ref, count_ref, near_ref, far_ref, ends_ref):
    positions, tcap = src_ref.shape

    def one(p, found):
        n_near, n_far = found
        count = count_ref[p, 0]
        for k in range(tcap):
            owner, place = split(src_ref[p, k], blocks)
            _, away = split(me + n_node - owner, n_node)
            code = (p * tcap + k) | (dst_ref[p, k] << 24)
            near_ref[n_near] = code | (place << 12)
            far_ref[n_far] = code | ((place + (away - 1) * blocks) << 12)
            live = k < count
            n_near = n_near + jnp.where(jnp.logical_and(live, away == 0), 1, 0)
            n_far = n_far + jnp.where(jnp.logical_and(live, away != 0), 1, 0)
        return n_near, n_far

    n_near, n_far = lax.fori_loop(0, positions, one, (jnp.int32(0), jnp.int32(0)))
    ends_ref[0] = n_near
    ends_ref[1] = n_far


def near_body(n_node, me_ref, src_ref, dst_ref, count_ref, perm_ref, prior_ref, bits_ref, qt_ref, k_ref, vt_ref, atts_ref, msgt_ref, m_ref, l_ref, a_ref, far_ref, ends_ref, near_s, *stage):
    build_lists(n_node, qt_ref.shape[0], me_ref[0], src_ref, dst_ref, count_ref, near_s, far_ref, ends_ref)
    m_ref[...] = jnp.full(m_ref.shape, FLOOR, F32)
    l_ref[...] = jnp.zeros(l_ref.shape, F32)
    a_ref[...] = jnp.zeros(a_ref.shape, F32)
    visit_tiles(near_s, ends_ref[0], src_ref.shape[1], perm_ref, prior_ref, bits_ref, qt_ref, k_ref, vt_ref, atts_ref, msgt_ref, m_ref, l_ref, a_ref, *stage)


def far_body(n_rel, tcap, far_ref, ends_ref, perm_ref, prior_ref, bits_ref, qt_ref, k_ref, vt_ref, atts_ref, msgt_ref, m_in, l_in, a_in, send_ref, m_ref, l_ref, a_ref, *stage):
    visit_tiles(far_ref, ends_ref[1], tcap, perm_ref, prior_ref, bits_ref, qt_ref, k_ref, vt_ref, atts_ref, msgt_ref, m_ref, l_ref, a_ref, *stage)
    heads, cols = prior_ref.shape[0], qt_ref.shape[1]
    blocks = a_ref.shape[0]
    n_head = blocks // n_rel
    for b in range(blocks):
        spot = (b % n_rel) * n_head + b // n_rel
        send_ref[spot, :cols, :] = a_ref[b].astype(BF)
        rows = []
        for value in (m_ref[b], l_ref[b]):
            rest = value
            for _ in range(3):
                piece = rest.astype(BF).astype(F32)
                rest = rest - piece
                rows += [piece[:, h * LANES : (h + 1) * LANES] for h in range(heads)]
        rows.append(jnp.zeros((TAIL - len(rows), LANES), F32))
        send_ref[spot, cols:, :] = jnp.concatenate(rows, axis=0).astype(BF)


def visit_tiles(
    list_ref, count, tcap, perm_ref, prior_ref, bits_ref, qt_ref, k_ref, vt_ref, atts_ref, msgt_ref, m_ref, l_ref, a_ref, q_s, w_s, v_s, t_s
):
    heads = prior_ref.shape[0]
    cols = qt_ref.shape[1]
    hd = cols // heads
    factor = 1.0 / math.sqrt(hd)
    q_s[...] = jnp.zeros(q_s.shape, BF)
    w_s[...] = jnp.zeros(w_s.shape, BF)
    v_s[...] = jnp.zeros(v_s.shape, BF)
    t_s[0] = jnp.full(t_s.shape[1:], FLOOR, F32)
    t_s[1] = jnp.zeros(t_s.shape[1:], F32)
    shift = 31 - lax.broadcasted_iota(jnp.int32, (32, LANES), 0)

    def read(index):
        code = list_ref[jnp.clip(index, 0, count - 1)]
        slot = code & 0xFFF
        return slot, (code >> 12) & 0xFFF, code >> 24, split(slot, tcap)[0]

    def by_head(left, right):
        return [
            jnp.dot(left[h], right[h * hd : (h + 1) * hd], preferred_element_type=F32) for h in range(heads)
        ]

    def visit(turn, carry):
        base = turn * GROUP
        sums, scores, messages, queries = [], [], [], []
        for g in range(GROUP):
            sums.append(
                [
                    jnp.dot(
                        v_s[g, h * hd : (h + 1) * hd, :],
                        w_s[g, :, h * LANES : (h + 1) * LANES],
                        preferred_element_type=F32,
                    )
                    for h in range(heads)
                ]
            )
        for g in range(GROUP):
            slot, src, dst, position = read(base - GROUP + g)
            scores.append(jnp.dot(k_ref[src], q_s[g], preferred_element_type=F32))
            messages.append(by_head(msgt_ref[position], vt_ref[src]))
        for g in range(GROUP):
            slot, src, dst, position = read(base + g)
            queries.append(by_head(atts_ref[position], qt_ref[dst]))
        for g in range(GROUP):
            slot, src, dst, position = read(base - 2 * GROUP + g)
            top, total = t_s[0, g], t_s[1, g]
            m_old = m_ref[dst]
            m_new = jnp.maximum(m_old, top)
            keep = jnp.exp(m_old - m_new)
            take = jnp.exp(top - m_new)
            m_ref[dst] = m_new
            l_ref[dst] = l_ref[dst] * keep + total * take
            for h in range(heads):
                lanes = slice(h * LANES, (h + 1) * LANES)
                rows = slice(h * hd, (h + 1) * hd)
                a_ref[dst, rows, :] = a_ref[dst, rows, :] * keep[:, lanes] + sums[g][h] * take[:, lanes]
        for g in range(GROUP):
            index = base - GROUP + g
            slot, src, dst, position = read(index)
            valid = jnp.logical_and(index >= 0, index < count)
            words = jnp.where(valid, bits_ref[slot], 0)
            parts = []
            for w in range(words.shape[0]):
                edge = (jnp.broadcast_to(words[w : w + 1], (32, LANES)) << shift) < 0
                for_heads = jnp.concatenate([edge] * heads, axis=1)
                parts.append(jnp.where(for_heads, scores[g][w * 32 : (w + 1) * 32], NEG))
            masked = jnp.concatenate(parts, axis=0)
            top = jnp.maximum(jnp.max(masked, axis=0, keepdims=True), FLOOR)
            weights = jnp.exp(masked - top)
            t_s[0, g] = top
            t_s[1, g] = jnp.sum(weights, axis=0, keepdims=True)
            w_s[g] = weights.astype(BF)
            for h in range(heads):
                v_s[g, h * hd : (h + 1) * hd, :] = messages[g][h].astype(BF)
        for g in range(GROUP):
            slot, src, dst, position = read(base + g)
            for h in range(heads):
                rows = slice(h * hd, (h + 1) * hd)
                scale = prior_ref[h, perm_ref[position]] * factor
                q_s[g, rows, h * LANES : (h + 1) * LANES] = (queries[g][h] * scale).astype(BF)
        return carry

    lax.fori_loop(0, jnp.where(count > 0, lax.div(count + GROUP - 1, GROUP) + 2, 0), visit, 0)


def finish_body(heads, n_rel, n_head, me_ref, skip_ref, got_ref, x_ref, kinds_ref, *refs):
    w_refs, out_ref = refs[:-1], refs[-1]
    cols = got_ref.shape[1] - TAIL
    hd = cols // heads
    types = w_refs[0].shape[0]
    hits = hits_of(kinds_ref[...], types)
    hidden = []
    for s in range(n_head):
        h_from = lax.rem(me_ref[0] + n_head - s, n_head)
        accs, tops, totals = [], [], []
        for z in range(n_rel):
            spot = z * n_head + h_from
            accs.append(got_ref[spot, :cols, :])
            tail = got_ref[spot, cols:, :].astype(F32)
            m = tail[0:heads] + tail[heads : 2 * heads] + tail[2 * heads : 3 * heads]
            tail = tail[3 * heads :]
            tops.append(m)
            totals.append(tail[0:heads] + tail[heads : 2 * heads] + tail[2 * heads : 3 * heads])
        top = functools.reduce(jnp.maximum, tops)
        scales = [jnp.exp(m - top) for m in tops]
        total = functools.reduce(jnp.add, [l * e for l, e in zip(totals, scales)])
        inverse = 1.0 / jnp.maximum(total, 1.0)
        rows = []
        for h in range(heads):
            acc = functools.reduce(
                jnp.add,
                [a[h * hd : (h + 1) * hd].astype(F32) * e[h : h + 1] for a, e in zip(accs, scales)],
            )
            rows.append(jax.nn.gelu(acc * inverse[h : h + 1]))
        hidden.append(jnp.concatenate(rows, axis=0).T.astype(BF))
    mixed = None
    for s in range(n_head):
        w = w_refs[s][...].reshape(types * cols, -1)
        spread_rows = jnp.concatenate([hidden[s] * hit.astype(BF) for hit in hits], axis=1)
        part = jnp.dot(spread_rows, w, preferred_element_type=F32)
        mixed = part if mixed is None else mixed + part
    gate = jnp.zeros((LANES, LANES), F32)
    for kind in range(types):
        gate = gate + hits[kind] * jax.nn.sigmoid(jnp.full((LANES, LANES), skip_ref[kind], F32))
    gate = jnp.concatenate([gate] * (mixed.shape[1] // LANES), axis=1)
    out_ref[...] = (gate * mixed + (1.0 - gate) * x_ref[...].astype(F32)).astype(BF)


def onchip(x):
    return pltpu.with_memory_space_constraint(x, pltpu.VMEM)


def offchip(x):
    return pltpu.with_memory_space_constraint(x, pltpu.HBM)


def shifted(n, s):
    return [(i, (i + s) % n) for i in range(n)]


def layer(
    features,
    node_type,
    w_query,
    w_key,
    w_value,
    rel_att,
    rel_msg,
    rel_prior,
    w_out,
    skip,
    rel_perm,
    tile_src,
    tile_dst,
    tile_bits,
    tile_count,
):
    node_rows, depth = features.shape
    n_rel = lax.axis_size("rel")
    n_node = lax.axis_size("node")
    n_head = lax.axis_size("head")
    heads = rel_prior.shape[1]
    types, _, cols = w_query.shape
    hd = cols // heads
    positions, tcap, block, words = tile_bits.shape
    blocks = node_rows // block
    slots = positions * tcap
    kinds = node_type.reshape(blocks, block)

    w_parts = [w_out] + [lax.ppermute(w_out, "head", shifted(n_head, s)) for s in range(1, n_head)]

    step = math.gcd(4, blocks)
    x_spec = pl.BlockSpec((step * block, depth), lambda i: (i, 0))
    kinds_spec = pl.BlockSpec((1, step, block), lambda i: (i, 0, 0))
    w_spec = pl.BlockSpec((types, depth, cols), lambda i: (0, 0, 0))
    b_spec = pl.BlockSpec((step, block, cols), lambda i: (i, 0, 0))
    bt_spec = pl.BlockSpec((step, cols, block), lambda i: (i, 0, 0))
    kinds_in = offchip(kinds.reshape(blocks // step, step, block))
    keys, values_t = pl.pallas_call(
        kv_body,
        grid=(blocks // step,),
        in_specs=[x_spec, kinds_spec, w_spec, w_spec],
        out_specs=[b_spec, bt_spec],
        out_shape=[
            pltpu.VMEM((blocks, block, cols), BF),
            pltpu.VMEM((blocks, cols, block), BF),
        ],
        compiler_params=SMALL,
        name="keys_values",
    )(offchip(features), kinds_in, offchip(w_key), offchip(w_value))

    far_keys = [lax.ppermute(keys, "node", shifted(n_node, s)) for s in range(1, n_node)]
    far_values = [lax.ppermute(values_t, "node", shifted(n_node, s)) for s in range(1, n_node)]

    d_spec = pl.BlockSpec((positions, heads, hd, hd), lambda i, perm: (0, 0, 0, 0))
    queries_t, atts, msgs_t = pl.pallas_call(
        q_body,
        grid_spec=pltpu.PrefetchScalarGridSpec(
            num_scalar_prefetch=1,
            grid=(blocks // step,),
            in_specs=[
                pl.BlockSpec((step * block, depth), lambda i, perm: (i, 0)),
                pl.BlockSpec((1, step, block), lambda i, perm: (i, 0, 0)),
                pl.BlockSpec((types, depth, cols), lambda i, perm: (0, 0, 0)),
                ANY,
                ANY,
            ],
            out_specs=[pl.BlockSpec((step, cols, block), lambda i, perm: (i, 0, 0)), d_spec, d_spec],
            scratch_shapes=[
                pltpu.VMEM((positions, heads, hd, hd), BF),
                pltpu.SemaphoreType.DMA((2, positions)),
            ],
        ),
        out_shape=[
            pltpu.VMEM((blocks, cols, block), BF),
            pltpu.VMEM((positions, heads, hd, hd), BF),
            pltpu.VMEM((positions, heads, hd, hd), BF),
        ],
        compiler_params=SMALL,
        name="queries",
    )(rel_perm, offchip(features), kinds_in, offchip(w_query), offchip(rel_att), offchip(rel_msg))

    me = lax.axis_index("node").reshape(1)
    prior = rel_prior.T
    bits = tile_bits.transpose(0, 1, 3, 2).reshape(slots, words, block)
    state_shapes = [
        pltpu.VMEM((blocks, 1, heads * block), F32),
        pltpu.VMEM((blocks, 1, heads * block), F32),
        pltpu.VMEM((blocks, cols, block), F32),
    ]
    stage = [
        pltpu.VMEM((GROUP, cols, heads * block), BF),
        pltpu.VMEM((GROUP, block, heads * block), BF),
        pltpu.VMEM((GROUP, cols, block), BF),
        pltpu.VMEM((2, GROUP, 1, heads * block), F32),
    ]
    shared = [onchip(x) for x in (bits, queries_t, atts, msgs_t)]
    *state, far_list, ends = pl.pallas_call(
        functools.partial(near_body, n_node),
        in_specs=[SMEM] * 6 + [VMEM] * 6,
        out_specs=[VMEM] * 3 + [SMEM] * 2,
        out_shape=state_shapes
        + [jax.ShapeDtypeStruct((slots,), jnp.int32), jax.ShapeDtypeStruct((2,), jnp.int32)],
        scratch_shapes=[pltpu.SMEM((slots,), jnp.int32)] + stage,
        compiler_params=SMALL,
        name="near_tiles",
    )(me, tile_src, tile_dst, tile_count, rel_perm, prior, *shared[:2], onchip(keys), onchip(values_t), *shared[2:])

    def joined(arrays):
        return onchip(arrays[0] if len(arrays) == 1 else jnp.concatenate(arrays, axis=0))

    send, *_ = pl.pallas_call(
        functools.partial(far_body, n_rel, tcap),
        in_specs=[SMEM] * 4 + [VMEM] * 9,
        out_specs=[VMEM] * 4,
        out_shape=[jax.ShapeDtypeStruct((blocks, cols + TAIL, block), BF)] + state_shapes,
        input_output_aliases={10: 1, 11: 2, 12: 3},
        scratch_shapes=stage,
        compiler_params=SMALL,
        name="far_tiles",
    )(far_list, ends, rel_perm, prior, *shared[:2], joined(far_keys), joined(far_values), *shared[2:], *state)

    got = lax.all_to_all(send, ("rel", "head"), 0, 0, tiled=True)

    spot = lax.axis_index("head") * n_rel + lax.axis_index("rel")
    own_rows = lax.dynamic_slice_in_dim(features, spot * block, block, 0)
    own_kinds = lax.dynamic_slice_in_dim(kinds, spot, 1, 0)
    finished = pl.pallas_call(
        functools.partial(finish_body, heads, n_rel, n_head),
        in_specs=[SMEM, SMEM] + [VMEM] * (3 + n_head),
        out_specs=VMEM,
        out_shape=jax.ShapeDtypeStruct((block, depth), BF),
        compiler_params=SMALL,
        name="finish",
    )(lax.axis_index("head").reshape(1), skip, *[onchip(x) for x in (got, own_rows, own_kinds, *w_parts)])
    return lax.all_gather(finished, "rel", axis=0, tiled=True)


def solution(mesh):
    in_specs = (
        P("node", None),
        P("node"),
        P(None, None, "head"),
        P(None, None, "head"),
        P(None, None, "head"),
        P(None, "head", None, None),
        P(None, "head", None, None),
        P(None, "head"),
        P(None, "head", None),
        P(),
        P("rel"),
        P("rel", "node"),
        P("rel", "node"),
        P("rel", "node", None, None),
        P("rel", "node"),
    )
    out_specs = P(("node", "head"), None)
    return jax.shard_map(layer, mesh=mesh, in_specs=in_specs, out_specs=out_specs, check_vma=False)
```
